8 devices in a mesh: batch: 1 (over z), time: 8 (over y, x, core).
Axes of the slice: x: 2, y: 2, z: 1, core: 2. Of those that a mesh axis runs over, the one named last changes fastest.
Arguments:
- latent: bfloat16 [16, 6, 128, 384], P(('batch', 'time'))
- conv_w: bfloat16 [4, 3, 3, 3, 384, 384], replicated
- conv_b: float32 [4, 384], replicated
- norm_g: float32 [5, 384], replicated
- norm_b: float32 [5, 384], replicated
- attn_w: bfloat16 [4, 384, 384], replicated
- attn_b: float32 [4, 384], replicated
Outputs:
- output: bfloat16 [16, 6, 128, 384], P(('batch', 'time'))
All inputs are finite; a program needn't handle non-finite values.
Results may differ from the reference program's by a relative error of at most 0.0124786.
Values are sent between devices in bfloat16 or wider.
A program may use at most 1 GiB of HBM per device.

```python
import jax
import jax.numpy as jnp
from jax import lax

FRAMES = 16
HEIGHT = 6
WIDTH = 128
CHANNELS = 384
GROUPS = 32
NORM_EPS = 1e-6


def setup_inputs(seed: int = 0, part: int = 0) -> dict:
    part_key = jax.random.fold_in(jax.random.key(seed), part)
    video_keys = jax.random.split(part_key, 4)
    weight_keys = jax.random.split(jax.random.key(seed + 1), 6)
    time_pos = jnp.arange(FRAMES, dtype=jnp.float32) / max(FRAMES - 1, 1) - 0.5
    time_slope = 1.4 + 0.4 * jax.random.uniform(video_keys[0], (), jnp.float32)
    frame_scale = jnp.exp(time_slope * time_pos)[:, None, None, None]
    chan_offset = jax.random.normal(video_keys[1], (CHANNELS,), jnp.float32)
    frame_mean = time_pos[:, None, None, None] * chan_offset
    shared_noise = jax.random.normal(video_keys[2], (1, HEIGHT, WIDTH, CHANNELS), jnp.float32)
    fresh_noise = jax.random.normal(video_keys[3], (FRAMES, HEIGHT, WIDTH, CHANNELS), jnp.float32)
    latent = frame_scale * (0.5 * shared_noise + 0.85 * fresh_noise) + frame_mean
    conv_w = jax.random.normal(weight_keys[0], (4, 3, 3, 3, CHANNELS, CHANNELS), jnp.float32) * (27 * CHANNELS) ** -0.5
    conv_b = 0.3 * jax.random.normal(weight_keys[1], (4, CHANNELS), jnp.float32)
    norm_g = 1.0 + 0.3 * jax.random.normal(weight_keys[2], (5, CHANNELS), jnp.float32)
    norm_b = 0.3 * jax.random.normal(weight_keys[3], (5, CHANNELS), jnp.float32)
    attn_w = jax.random.normal(weight_keys[4], (4, CHANNELS, CHANNELS), jnp.float32) * CHANNELS ** -0.5
    attn_b = 0.3 * jax.random.normal(weight_keys[5], (4, CHANNELS), jnp.float32)
    return {"latent": latent.astype(jnp.bfloat16), "conv_w": conv_w.astype(jnp.bfloat16), "conv_b": conv_b, "norm_g": norm_g, "norm_b": norm_b, "attn_w": attn_w.astype(jnp.bfloat16), "attn_b": attn_b}


def group_norm(feature, norm_gain, norm_shift):
    values_f = feature.astype(jnp.float32)
    grouped = values_f.reshape(FRAMES, HEIGHT, WIDTH, GROUPS, CHANNELS // GROUPS)
    elem_count = FRAMES * HEIGHT * WIDTH * (CHANNELS // GROUPS)
    group_mean = jnp.sum(grouped, axis=(0, 1, 2, 4)) / elem_count
    group_sq = jnp.sum(grouped * grouped, axis=(0, 1, 2, 4)) / elem_count
    inv_std = lax.rsqrt(group_sq - group_mean * group_mean + NORM_EPS)
    mean_full = jnp.repeat(group_mean, CHANNELS // GROUPS)
    scale_full = jnp.repeat(inv_std, CHANNELS // GROUPS) * norm_gain
    return (values_f - mean_full) * scale_full + norm_shift


def causal_conv(activation, kernel, conv_bias):
    padded = jnp.concatenate([activation[:1], activation[:1], activation], axis=0)
    conv_out = lax.conv_general_dilated(padded[None].astype(jnp.float32), kernel.astype(jnp.float32), (1, 1, 1), ((0, 0), (1, 1), (1, 1)), dimension_numbers=("NDHWC", "DHWIO", "NDHWC"))
    return (conv_out[0] + conv_bias).astype(jnp.bfloat16)


def resnet_block(feature, conv_w, conv_b, norm_g, norm_b, norm_first, conv_first):
    activation = jax.nn.silu(group_norm(feature, norm_g[norm_first], norm_b[norm_first])).astype(jnp.bfloat16)
    branch = causal_conv(activation, conv_w[conv_first], conv_b[conv_first])
    activation = jax.nn.silu(group_norm(branch, norm_g[norm_first + 1], norm_b[norm_first + 1])).astype(jnp.bfloat16)
    branch = causal_conv(activation, conv_w[conv_first + 1], conv_b[conv_first + 1])
    return (feature.astype(jnp.float32) + branch.astype(jnp.float32)).astype(jnp.bfloat16)


def spatial_attention(feature, norm_gain, norm_shift, attn_w, attn_b):
    normed = group_norm(feature, norm_gain, norm_shift).astype(jnp.bfloat16)
    tokens = normed.reshape(FRAMES, HEIGHT * WIDTH, CHANNELS)
    score_scale = CHANNELS ** -0.5

    def one_frame(frame_tok):
        queries = (jnp.dot(frame_tok, attn_w[0], preferred_element_type=jnp.float32) + attn_b[0]).astype(jnp.bfloat16)
        keys_t = (jnp.dot(frame_tok, attn_w[1], preferred_element_type=jnp.float32) + attn_b[1]).astype(jnp.bfloat16)
        values_t = (jnp.dot(frame_tok, attn_w[2], preferred_element_type=jnp.float32) + attn_b[2]).astype(jnp.bfloat16)
        scores = jnp.dot(queries, keys_t.T, preferred_element_type=jnp.float32) * score_scale
        attn_probs = jax.nn.softmax(scores, axis=-1).astype(jnp.bfloat16)
        mixed_val = jnp.dot(attn_probs, values_t, preferred_element_type=jnp.float32).astype(jnp.bfloat16)
        return (jnp.dot(mixed_val, attn_w[3], preferred_element_type=jnp.float32) + attn_b[3]).astype(jnp.bfloat16)

    projected = lax.map(one_frame, tokens).reshape(feature.shape)
    return (feature.astype(jnp.float32) + projected.astype(jnp.float32)).astype(jnp.bfloat16)


def reference(latent, conv_w, conv_b, norm_g, norm_b, attn_w, attn_b):
    feature = resnet_block(latent, conv_w, conv_b, norm_g, norm_b, 0, 0)
    feature = spatial_attention(feature, norm_g[2], norm_b[2], attn_w, attn_b)
    return resnet_block(feature, conv_w, conv_b, norm_g, norm_b, 3, 2)
```

```python
import functools

import jax
import jax.numpy as jnp
from jax import lax
from jax.experimental import pallas as pl
from jax.experimental.pallas import tpu as pltpu
from jax.sharding import PartitionSpec as P

GROUPS = 32
NORM_EPS = 1e-6
MESH = pl.DeviceIdType.MESH


def dot(a, b):
    return jnp.dot(a, b, preferred_element_type=jnp.float32)


def block_kernel(
    n, height, width, chans,
    latent, conv_w, conv_b, norm_g, norm_b, attn_w, attn_b, out,
    wbuf, awbuf, cbuf, gbuf, bbuf, abuf, umap, src, xres, land, acc, qkv, stat_out, stat_in,
    w_sem, p_sem, x_sem, o_sem, halo_send, halo_recv, st_send, st_recv,
):
    pos = height * width
    taps = 27
    lanes = chans // 128
    group = chans // GROUPS
    elems = n * 2 * pos * group
    me = lax.axis_index("time")
    inner = lax.min(me, 1)
    slot_m1, slot_m2 = 2 - inner, 2 - 2 * inner

    def x_copy(f):
        return pltpu.make_async_copy(latent.at[f], src.at[f], x_sem.at[f])

    def w_copy(k):
        return pltpu.make_async_copy(conv_w.at[k], wbuf.at[k], w_sem.at[k])

    small = [
        pltpu.make_async_copy(a, b, p_sem.at[i])
        for i, (a, b) in enumerate([(norm_g, gbuf), (norm_b, bbuf), (conv_b, cbuf), (attn_b, abuf)])
    ]
    aw_copy = pltpu.make_async_copy(attn_w, awbuf, p_sem.at[4])
    for f in range(2):
        x_copy(f).start()
    for c in small:
        c.start()
    for k in range(4):
        w_copy(k).start()
    aw_copy.start()

    barrier = pltpu.get_barrier_semaphore()
    for d in range(1, n):
        pl.semaphore_signal(barrier, inc=1, device_id={"time": lax.rem(me + d, n)}, device_id_type=MESH)

    zero_row = jnp.zeros((width, chans), jnp.bfloat16)
    for s in range(4):
        umap[s, 0:width, :] = zero_row
        umap[s, width + pos : 2 * width + pos, :] = zero_row

    def put_stats(index, s1, s2):
        rows = [jnp.sum(s[:, 128 * b : 128 * b + 128], axis=0, keepdims=True) for s in (s1, s2) for b in range(lanes)]
        rows.append(jnp.zeros((8 - 2 * lanes, 128), jnp.float32))
        stat_out[index] = jnp.concatenate(rows, axis=0)

    def add_stats(carry, v):
        s1, s2 = carry
        t = v.reshape(v.shape[0] // 8, 8, v.shape[1])
        return s1 + jnp.sum(t, axis=0), s2 + jnp.sum(t * t, axis=0)

    zero_stats = (jnp.zeros((8, chans), jnp.float32),) * 2

    def stat_copy(index, d):
        return pltpu.make_async_remote_copy(
            src_ref=stat_out.at[index],
            dst_ref=stat_in.at[index, me],
            send_sem=st_send.at[index, d],
            recv_sem=st_recv.at[index, d],
            device_id={"time": lax.rem(me + d, n)},
            device_id_type=MESH,
        )

    def norm_params(index):
        for d in range(1, n):
            stat_copy(index, d).start()
        stat_in[index, me] = stat_out[index]
        for d in range(1, n):
            stat_copy(index, d).wait()
        total = stat_in[index, 0]
        for d in range(1, n):
            total = total + stat_in[index, d]
        lane = lax.broadcasted_iota(jnp.int32, (8, 128), 1)
        chan = lane + 128 * lax.rem(lax.broadcasted_iota(jnp.int32, (8, 128), 0), lanes)
        place = lax.rem(chan, group)
        sums = jnp.zeros((8, 128), jnp.float32)
        for s in range(1 - group, group):
            moved = pltpu.roll(total, (-s) % 128, 1) if s else total
            if s > 0:
                moved = jnp.where(lane >= 128 - s, pltpu.roll(moved, 7, 0), moved)
            elif s < 0:
                moved = jnp.where(lane < -s, pltpu.roll(moved, 1, 0), moved)
            sums = sums + jnp.where((place + s >= 0) & (place + s < group), moved, 0.0)
        mean = jnp.concatenate([sums[b : b + 1] for b in range(lanes)], axis=1) / elems
        square = jnp.concatenate([sums[lanes + b : lanes + b + 1] for b in range(lanes)], axis=1) / elems
        scale = lax.rsqrt(square - mean * mean + NORM_EPS) * gbuf[pl.ds(index, 1), :]
        return mean, scale, bbuf[pl.ds(index, 1), :]

    def normed(v, params):
        mean, scale, shift = params
        return (v.astype(jnp.float32) - mean) * scale + shift

    def activate(v, params):
        y = 0.5 * normed(v, params)
        return (y + y * jnp.tanh(y)).astype(jnp.bfloat16)

    def fill(slot, read, params):
        def row(i, _):
            at = pl.multiple_of(i * width, width)
            umap[slot, pl.ds(at + width, width), :] = activate(read(at), params)
            return 0

        lax.fori_loop(0, height, row, 0)

    def halo_copy(k, f):
        return pltpu.make_async_remote_copy(
            src_ref=src.at[f],
            dst_ref=land.at[k, f],
            send_sem=halo_send.at[k, f],
            recv_sem=halo_recv.at[k, f],
            device_id={"time": lax.min(me + 1, n - 1)},
            device_id_type=MESH,
        )

    def send_halo(k, f):
        @pl.when(me < n - 1)
        def _():
            halo_copy(k, f).start()

    def lhs(slot):
        return jnp.concatenate([umap[slot, d * width : d * width + pos, :] for d in range(3)], axis=1)

    def rhs(k, a, e):
        return jnp.concatenate([wbuf[k, a * 9 + d * 3 + e] for d in range(3)], axis=0)

    def both_outs(k, slot, a0, first):
        def step(e, _):
            part = dot(lhs(slot), jnp.concatenate([rhs(k, a0, e), rhs(k, a0 - 1, e)], axis=1))
            acc[e] = part if first else acc[e] + part
            return 0

        lax.fori_loop(0, 3, step, 0)

    def one_out(k, slot, a, o):
        part = dot(lhs(slot), jnp.concatenate([rhs(k, a, e) for e in range(3)], axis=1))
        for e in range(3):
            acc[e, :, o * chans : (o + 1) * chans] += part[:, e * chans : (e + 1) * chans]

    def finish(k, o, stats):
        column = lax.broadcasted_iota(jnp.int32, (width, 1), 0)
        bias = cbuf[pl.ds(k, 1), :]
        odd = lax.rem(k, 2) == 1

        def row(i, carry):
            at = pl.ds(pl.multiple_of(i * width, width), width)
            cols = slice(o * chans, (o + 1) * chans)
            left = jnp.where(column == 0, 0.0, pltpu.roll(acc[0, at, cols], 1, 0))
            right = jnp.where(column == width - 1, 0.0, pltpu.roll(acc[2, at, cols], width - 1, 0))
            h = (acc[1, at, cols] + left + right + bias).astype(jnp.bfloat16).astype(jnp.float32)
            old = xres[o, at, :]
            new = jnp.where(odd, h + old.astype(jnp.float32), h).astype(jnp.bfloat16)
            src[o, at, :] = new
            xres[o, at, :] = jnp.where(odd, new, old)
            return add_stats(carry, new.astype(jnp.float32))

        return lax.fori_loop(0, height, row, stats)

    def out_copy(f):
        return pltpu.make_async_copy(src.at[f], out.at[f], o_sem.at[f])

    def attention():
        params = norm_params(2)
        aw_copy.wait()
        part_rows = pos // 3

        def frame(t, carry):
            f = 1 - t

            def project(i, _):
                at = pl.ds(pl.multiple_of(i * part_rows, part_rows), part_rows)
                a = normed(xres[f, at, :], params).astype(jnp.bfloat16)
                w = jnp.concatenate([awbuf[0], awbuf[1], awbuf[2]], axis=1)
                b = jnp.concatenate([abuf[j : j + 1] for j in range(3)], axis=1)
                qkv[at, :] = (dot(a, w) + b).astype(jnp.bfloat16)
                return 0

            lax.fori_loop(0, 3, project, 0)

            def attend(i, carry):
                at = pl.ds(pl.multiple_of(i * part_rows, part_rows), part_rows)
                scores = lax.dot_general(
                    qkv[at, 0:chans], qkv[:, chans : 2 * chans], (((1,), (1,)), ((), ())), preferred_element_type=jnp.float32
                ) * chans ** -0.5
                top = jnp.max(scores, axis=1, keepdims=True)
                e = jnp.exp(scores - top)
                p = (e / jnp.sum(e, axis=1, keepdims=True)).astype(jnp.bfloat16)
                o = dot(p, qkv[:, 2 * chans : 3 * chans]).astype(jnp.bfloat16)
                h = (dot(o, awbuf[3]) + abuf[3:4]).astype(jnp.bfloat16)
                new = (xres[f, at, :].astype(jnp.float32) + h.astype(jnp.float32)).astype(jnp.bfloat16)
                src[f, at, :] = new
                xres[f, at, :] = new
                return add_stats(carry, new.astype(jnp.float32))

            carry = lax.fori_loop(0, 3, attend, carry)
            send_halo(2, f)
            return carry

        put_stats(3, *lax.fori_loop(0, 2, frame, zero_stats))

    for f in range(2):
        x_copy(f).wait()

    def first_row(i, carry):
        for f in range(2):
            at = pl.ds(pl.multiple_of(i * width, width), width)
            v = src[f, at, :]
            xres[f, at, :] = v
            carry = add_stats(carry, v.astype(jnp.float32))
        return carry

    put_stats(0, *lax.fori_loop(0, height, first_row, zero_stats))
    for c in small:
        c.wait()
    pl.semaphore_wait(barrier, n - 1)
    for f in (1, 0):
        send_halo(0, f)

    def stage(k, _):
        index = k + lax.div(k, 2)
        params = norm_params(index)
        for f in range(2):
            fill(2 + f, lambda at: src[f, pl.ds(at, width), :], params)
        w_copy(k).wait()
        both_outs(k, 2, 2, True)
        one_out(k, 3, 2, 1)

        @pl.when(me > 0)
        def _():
            halo_copy(k, 1).wait_recv()
            fill(1, lambda at: land[k, 1, pl.ds(at, width), :], params)

        both_outs(k, slot_m1, 1, False)

        @pl.when(me < n - 1)
        def _():
            halo_copy(k, 1).wait_send()

        stats = finish(k, 1, zero_stats)

        @pl.when(lax.rem(k, 2) == 0)
        def _():
            send_halo(k + 1, 1)

        @pl.when(k == 3)
        def _():
            out_copy(1).start()

        @pl.when(me > 0)
        def _():
            halo_copy(k, 0).wait_recv()
            fill(0, lambda at: land[k, 0, pl.ds(at, width), :], params)

        one_out(k, slot_m2, 0, 0)

        @pl.when(me < n - 1)
        def _():
            halo_copy(k, 0).wait_send()

        stats = finish(k, 0, stats)

        @pl.when(lax.rem(k, 2) == 0)
        def _():
            send_halo(k + 1, 0)

        @pl.when(k == 3)
        def _():
            out_copy(0).start()

        put_stats(lax.min(index + 1, 4), *stats)

        @pl.when(k == 1)
        def _():
            attention()

        return 0

    lax.fori_loop(0, 4, stage, 0)
    for f in range(2):
        out_copy(f).wait()


def solution(mesh):
    n = mesh.shape["time"]
    video_spec = P(("batch", "time"), None, None, None)

    def device_body(latent, conv_w, conv_b, norm_g, norm_b, attn_w, attn_b):
        frames, height, width, chans = latent.shape
        pos = height * width
        bf16, f32 = jnp.bfloat16, jnp.float32
        out = pl.pallas_call(
            functools.partial(block_kernel, n, height, width, chans),
            out_shape=jax.ShapeDtypeStruct((frames, pos, chans), bf16),
            in_specs=[pl.BlockSpec(memory_space=pl.ANY)] * 7,
            out_specs=pl.BlockSpec(memory_space=pl.ANY),
            scratch_shapes=[
                pltpu.VMEM((4, 27, chans, chans), bf16),
                pltpu.VMEM((4, chans, chans), bf16),
                pltpu.VMEM((4, chans), f32),
                pltpu.VMEM((5, chans), f32),
                pltpu.VMEM((5, chans), f32),
                pltpu.VMEM((4, chans), f32),
                pltpu.VMEM((4, pos + 2 * width, chans), bf16),
                pltpu.VMEM((2, pos, chans), bf16),
                pltpu.VMEM((2, pos, chans), bf16),
                pltpu.VMEM((4, 2, pos, chans), bf16),
                pltpu.VMEM((3, pos, 2 * chans), f32),
                pltpu.VMEM((pos, 3 * chans), bf16),
                pltpu.VMEM((5, 8, 128), f32),
                pltpu.VMEM((5, n, 8, 128), f32),
                pltpu.SemaphoreType.DMA((4,)),
                pltpu.SemaphoreType.DMA((5,)),
                pltpu.SemaphoreType.DMA((2,)),
                pltpu.SemaphoreType.DMA((2,)),
                pltpu.SemaphoreType.DMA((4, 2)),
                pltpu.SemaphoreType.DMA((4, 2)),
                pltpu.SemaphoreType.DMA((5, n)),
                pltpu.SemaphoreType.DMA((5, n)),
            ],
            compiler_params=pltpu.CompilerParams(collective_id=0, has_side_effects=True, vmem_limit_bytes=67043328),
            name="mid_block",
        )(latent.reshape(frames, pos, chans), conv_w.reshape(4, 27, chans, chans), conv_b, norm_g, norm_b, attn_w, attn_b)
        return out.reshape(latent.shape)

    return jax.shard_map(device_body, mesh=mesh, in_specs=(video_spec, P(), P(), P(), P(), P(), P()), out_specs=video_spec, check_vma=False)
```

```python
import functools

import jax
import jax.numpy as jnp
from jax import lax
from jax.experimental import pallas as pl
from jax.experimental.pallas import tpu as pltpu
from jax.sharding import PartitionSpec as P

GROUPS = 32
NORM_EPS = 1e-6
MESH = pl.DeviceIdType.MESH


def dot(a, b):
    return jnp.dot(a, b, preferred_element_type=jnp.float32)


def copy_kernel(a, out, sem):
    c = pltpu.make_async_copy(a, out, sem)
    c.start()
    c.wait()


def block_kernel(
    n, height, width, chans,
    latent, conv_w, conv_b, norm_g, norm_b, attn_w, attn_b, out,
    wbuf, awbuf, cbuf, gbuf, bbuf, abuf, u_m2, u_m1, u_0, u_1, src, xres, land, acc, qkv, stat_out, stat_in,
    w_sem, p_sem, x_sem, halo_send, halo_recv, st_send, st_recv,
):
    pos = height * width
    taps = 27
    lanes = chans // 128
    group = chans // GROUPS
    elems = n * 2 * pos * group
    me = lax.axis_index("time")
    umaps = (u_m2, u_m1, u_0, u_1)

    def x_copy(f):
        return pltpu.make_async_copy(latent.at[f], src.at[f], x_sem.at[f])

    def w_copy(k):
        return pltpu.make_async_copy(conv_w.at[k], wbuf.at[k], w_sem.at[k])

    small = [
        pltpu.make_async_copy(a, b, p_sem.at[i])
        for i, (a, b) in enumerate([(norm_g, gbuf), (norm_b, bbuf), (conv_b, cbuf), (attn_b, abuf)])
    ]
    aw_copy = pltpu.make_async_copy(attn_w, awbuf, p_sem.at[4])
    for f in range(2):
        x_copy(f).start()
    for c in small:
        c.start()
    for k in range(4):
        w_copy(k).start()
    aw_copy.start()

    barrier = pltpu.get_barrier_semaphore()
    for d in range(1, n):
        pl.semaphore_signal(barrier, inc=1, device_id={"time": lax.rem(me + d, n)}, device_id_type=MESH)

    zero_row = jnp.zeros((width, chans), jnp.bfloat16)
    for u in umaps:
        u[0:width, :] = zero_row
        u[width + pos : 2 * width + pos, :] = zero_row

    def put_stats(index, s1, s2):
        rows = [jnp.sum(s[:, 128 * b : 128 * b + 128], axis=0, keepdims=True) for s in (s1, s2) for b in range(lanes)]
        rows.append(jnp.zeros((8 - 2 * lanes, 128), jnp.float32))
        stat_out[index] = jnp.concatenate(rows, axis=0)

    def add_stats(carry, v):
        s1, s2 = carry
        t = v.reshape(v.shape[0] // 8, 8, v.shape[1])
        return s1 + jnp.sum(t, axis=0), s2 + jnp.sum(t * t, axis=0)

    zero_stats = (jnp.zeros((8, chans), jnp.float32),) * 2

    def stat_copy(index, d):
        return pltpu.make_async_remote_copy(
            src_ref=stat_out.at[index],
            dst_ref=stat_in.at[index, me],
            send_sem=st_send.at[index, d],
            recv_sem=st_recv.at[index, d],
            device_id={"time": lax.rem(me + d, n)},
            device_id_type=MESH,
        )

    def norm_params(index, sent=None):
        for d in range(1, n):
            stat_copy(index, d).start()
        if sent is not None:
            sent()
        stat_in[index, me] = stat_out[index]
        for d in range(1, n):
            stat_copy(index, d).wait()
        total = stat_in[index, 0]
        for d in range(1, n):
            total = total + stat_in[index, d]
        lane = lax.broadcasted_iota(jnp.int32, (8, 128), 1)
        chan = lane + 128 * lax.rem(lax.broadcasted_iota(jnp.int32, (8, 128), 0), lanes)
        place = lax.rem(chan, group)
        sums = jnp.zeros((8, 128), jnp.float32)
        for s in range(1 - group, group):
            moved = pltpu.roll(total, (-s) % 128, 1) if s else total
            if s > 0:
                moved = jnp.where(lane >= 128 - s, pltpu.roll(moved, 7, 0), moved)
            elif s < 0:
                moved = jnp.where(lane < -s, pltpu.roll(moved, 1, 0), moved)
            sums = sums + jnp.where((place + s >= 0) & (place + s < group), moved, 0.0)
        mean = jnp.concatenate([sums[b : b + 1] for b in range(lanes)], axis=1) / elems
        square = jnp.concatenate([sums[lanes + b : lanes + b + 1] for b in range(lanes)], axis=1) / elems
        scale = lax.rsqrt(square - mean * mean + NORM_EPS) * gbuf[pl.ds(index, 1), :]
        return mean, scale, bbuf[pl.ds(index, 1), :]

    def normed(v, params):
        mean, scale, shift = params
        return (v.astype(jnp.float32) - mean) * scale + shift

    def activate(v, params):
        y = 0.5 * normed(v, params)
        return (y + y * jnp.tanh(y)).astype(jnp.bfloat16)

    def fill(u, read, params):
        for i in range(height):
            u[(i + 1) * width : (i + 2) * width, :] = activate(read(i * width), params)

    def own(f):
        return lambda at: src[f, at : at + width, :]

    def halo(k, f):
        return lambda at: jnp.where(me == 0, src[0, at : at + width, :], land[k, f, at : at + width, :])

    half = pos // 2
    parts = ((1, 0, half), (1, half, half), (0, 0, pos))

    def halo_copy(k, part):
        f, at, rows = parts[part]
        return pltpu.make_async_remote_copy(
            src_ref=src.at[f, pl.ds(at, rows)],
            dst_ref=land.at[k, f, pl.ds(at, rows)],
            send_sem=halo_send.at[k, part],
            recv_sem=halo_recv.at[k, part],
            device_id={"time": lax.min(me + 1, n - 1)},
            device_id_type=MESH,
        )

    def send_halo(k, *which):
        @pl.when(me < n - 1)
        def _():
            for part in which:
                halo_copy(k, part).start()

    def halo_sent(k, *which):
        @pl.when(me < n - 1)
        def _():
            for part in which:
                halo_copy(k, part).wait_send()

    def halo_here(k, *which):
        @pl.when(me > 0)
        def _():
            for part in which:
                halo_copy(k, part).wait_recv()

    column = lax.broadcasted_iota(jnp.int32, (width, 1), 0)

    spans = ((1, height - 1, (0, 1, 2)), (0, 1, (1, 2)), (height - 1, height, (0, 1)))

    def lhs(span, *us):
        top, end, ds = span
        return jnp.concatenate([u[(d + top) * width : (d + end) * width, :] for u in us for d in ds], axis=1)

    def rhs(span, k, a, e):
        return jnp.concatenate([wbuf[k, a * 9 + d * 3 + e] for d in span[2]], axis=0)

    def add_shifted(span, part, e, cols, first=False):
        for i in range(span[0], span[1]):
            at = slice(i * width, (i + 1) * width)
            v = part[(i - span[0]) * width : (i - span[0] + 1) * width]
            if e == 0:
                v = jnp.where(column == 0, 0.0, pltpu.roll(v, 1, 0))
            elif e == 2:
                v = jnp.where(column == width - 1, 0.0, pltpu.roll(v, width - 1, 0))
            acc[at, cols] = v if first else acc[at, cols] + v

    outs = [slice(o * chans, (o + 1) * chans) for o in range(2)]

    def one_out(k, u, a, o, first):
        for span in spans:
            part = dot(lhs(span, u), jnp.concatenate([rhs(span, k, a, e) for e in range(3)], axis=1))
            for e in range(3):
                add_shifted(span, part[:, e * chans : (e + 1) * chans], e, outs[o], first and e == 0)

    def both_outs(k, e, *frames, first=False):
        for span in spans:
            w = [jnp.concatenate([rhs(span, k, 2 - f, e), rhs(span, k, 1 - f, e)], axis=1) for f in frames]
            part = dot(lhs(span, *((u_0, u_m1)[f] for f in frames)), jnp.concatenate(w, axis=0))
            for o in range(2):
                add_shifted(span, part[:, outs[o]], e, outs[o], o == 0 and first)

    def finish(k, o, stats):
        bias = cbuf[pl.ds(k, 1), :]
        odd = lax.rem(k, 2) == 1
        for i in range(height):
            at = slice(i * width, (i + 1) * width)
            h = (acc[at, outs[o]] + bias).astype(jnp.bfloat16).astype(jnp.float32)
            old = xres[o, at, :]
            new = jnp.where(odd, h + old.astype(jnp.float32), h).astype(jnp.bfloat16)
            src[o, at, :] = new
            xres[o, at, :] = jnp.where(odd, new, old)
            stats = add_stats(stats, new.astype(jnp.float32))
        return stats

    def attention():
        params = norm_params(2)
        aw_copy.wait()
        part_rows = pos // 3

        def frame(t, carry):
            f = 1 - t

            def project(i, _):
                at = pl.ds(pl.multiple_of(i * part_rows, part_rows), part_rows)
                a = normed(xres[f, at, :], params).astype(jnp.bfloat16)
                w = jnp.concatenate([awbuf[0], awbuf[1], awbuf[2]], axis=1)
                b = jnp.concatenate([abuf[j : j + 1] for j in range(3)], axis=1)
                qkv[at, :] = (dot(a, w) + b).astype(jnp.bfloat16)
                return 0

            lax.fori_loop(0, 3, project, 0)

            def attend(i, carry):
                at = pl.ds(pl.multiple_of(i * part_rows, part_rows), part_rows)
                scores = lax.dot_general(
                    qkv[at, 0:chans], qkv[:, chans : 2 * chans], (((1,), (1,)), ((), ())), preferred_element_type=jnp.float32
                ) * chans ** -0.5
                top = jnp.max(scores, axis=1, keepdims=True)
                e = jnp.exp(scores - top)
                p = (e / jnp.sum(e, axis=1, keepdims=True)).astype(jnp.bfloat16)
                o = dot(p, qkv[:, 2 * chans : 3 * chans]).astype(jnp.bfloat16)
                h = (dot(o, awbuf[3]) + abuf[3:4]).astype(jnp.bfloat16)
                new = (xres[f, at, :].astype(jnp.float32) + h.astype(jnp.float32)).astype(jnp.bfloat16)
                src[f, at, :] = new
                xres[f, at, :] = new
                return add_stats(carry, new.astype(jnp.float32))

            carry = lax.fori_loop(0, 3, attend, carry)

            @pl.when(t == 0)
            def _():
                send_halo(2, 0)

            return carry

        put_stats(3, *lax.fori_loop(0, 2, frame, zero_stats))

    for f in range(2):
        x_copy(f).wait()

    def first_row(i, carry):
        for f in range(2):
            at = pl.ds(pl.multiple_of(i * width, width), width)
            v = src[f, at, :]
            xres[f, at, :] = v
            carry = add_stats(carry, v.astype(jnp.float32))
        return carry

    put_stats(0, *lax.fori_loop(0, height, first_row, zero_stats))
    for c in small:
        c.wait()
    pl.semaphore_wait(barrier, n - 1)
    send_halo(0, 0)

    def stage(k, _):
        index = k + lax.div(k, 2)
        params = norm_params(index, lambda: send_halo(k, 1, 2))
        fill(u_1, own(1), params)
        w_copy(k).wait()
        fill(u_0, own(0), params)
        one_out(k, u_1, 2, 1, True)
        halo_here(k, 0, 1)
        both_outs(k, 0, 0, first=True)
        fill(u_m1, halo(k, 1), params)
        both_outs(k, 0, 1)
        both_outs(k, 1, 0, 1)
        halo_here(k, 2)
        fill(u_m2, halo(k, 0), params)
        both_outs(k, 2, 0, 1)
        halo_sent(k, 0, 1)
        stats = finish(k, 1, zero_stats)

        @pl.when(lax.rem(k, 2) == 0)
        def _():
            send_halo(k + 1, 0)

        one_out(k, u_m2, 0, 0, False)
        halo_sent(k, 2)
        stats = finish(k, 0, stats)
        put_stats(lax.min(index + 1, 4), *stats)

        @pl.when(k == 1)
        def _():
            attention()

        return 0

    lax.fori_loop(0, 4, stage, 0)
    out[...] = src[...]


def solution(mesh):
    n = mesh.shape["time"]
    video_spec = P(("batch", "time"), None, None, None)

    def device_body(latent, conv_w, conv_b, norm_g, norm_b, attn_w, attn_b):
        frames, height, width, chans = latent.shape
        pos = height * width
        bf16, f32 = jnp.bfloat16, jnp.float32
        out = pl.pallas_call(
            functools.partial(block_kernel, n, height, width, chans),
            out_shape=jax.ShapeDtypeStruct((frames, pos, chans), bf16),
            in_specs=[pl.BlockSpec(memory_space=pltpu.HBM)] * 7,
            out_specs=pl.BlockSpec(memory_space=pltpu.VMEM),
            scratch_shapes=[
                pltpu.VMEM((4, 27, chans, chans), bf16),
                pltpu.VMEM((4, chans, chans), bf16),
                pltpu.VMEM((4, chans), f32),
                pltpu.VMEM((5, chans), f32),
                pltpu.VMEM((5, chans), f32),
                pltpu.VMEM((4, chans), f32),
                pltpu.VMEM((pos + 2 * width, chans), bf16),
                pltpu.VMEM((pos + 2 * width, chans), bf16),
                pltpu.VMEM((pos + 2 * width, chans), bf16),
                pltpu.VMEM((pos + 2 * width, chans), bf16),
                pltpu.VMEM((2, pos, chans), bf16),
                pltpu.VMEM((2, pos, chans), bf16),
                pltpu.VMEM((4, 2, pos, chans), bf16),
                pltpu.VMEM((pos, 2 * chans), f32),
                pltpu.VMEM((pos, 3 * chans), bf16),
                pltpu.VMEM((5, 8, 128), f32),
                pltpu.VMEM((5, n, 8, 128), f32),
                pltpu.SemaphoreType.DMA((4,)),
                pltpu.SemaphoreType.DMA((5,)),
                pltpu.SemaphoreType.DMA((2,)),
                pltpu.SemaphoreType.DMA((4, 3)),
                pltpu.SemaphoreType.DMA((4, 3)),
                pltpu.SemaphoreType.DMA((5, n)),
                pltpu.SemaphoreType.DMA((5, n)),
            ],
            compiler_params=pltpu.CompilerParams(collective_id=0, has_side_effects=True, vmem_limit_bytes=55000000),
            name="mid_block",
        )(latent.reshape(frames, pos, chans), conv_w.reshape(4, 27, chans, chans), conv_b, norm_g, norm_b, attn_w, attn_b)
        out = pl.pallas_call(
            copy_kernel,
            out_shape=jax.ShapeDtypeStruct((frames, pos, chans), bf16),
            in_specs=[pl.BlockSpec(memory_space=pltpu.VMEM)],
            out_specs=pl.BlockSpec(memory_space=pl.ANY),
            scratch_shapes=[pltpu.SemaphoreType.DMA],
            name="write_out",
        )(out)
        return out.reshape(latent.shape)

    return jax.shard_map(device_body, mesh=mesh, in_specs=(video_spec, P(), P(), P(), P(), P(), P()), out_specs=video_spec, check_vma=False)
```

```python
import functools

import jax
import jax.numpy as jnp
from jax import lax
from jax.experimental import pallas as pl
from jax.experimental.pallas import tpu as pltpu
from jax.sharding import PartitionSpec as P

GROUPS = 32
NORM_EPS = 1e-6
MESH = pl.DeviceIdType.MESH


def dot(a, b):
    return jnp.dot(a, b, preferred_element_type=jnp.float32)


def copy_kernel(a, out, sem):
    c = pltpu.make_async_copy(a, out, sem)
    c.start()
    c.wait()


def block_kernel(
    n, height, width, chans,
    latent, conv_w, conv_b, norm_g, norm_b, attn_w, attn_b, out,
    wbuf, awbuf, cbuf, gbuf, bbuf, abuf, u_m2, u_m1, u_0, u_1, src, xres, land, acc, qkv, stat_out, stat_in,
    w_sem, p_sem, x_sem, halo_send, halo_recv, st_send, st_recv,
):
    pos = height * width
    taps = 27
    lanes = chans // 128
    group = chans // GROUPS
    elems = n * 2 * pos * group
    me = lax.axis_index("time")
    umaps = (u_m2, u_m1, u_0, u_1)

    def x_copy(f):
        return pltpu.make_async_copy(latent.at[f], src.at[f], x_sem.at[f])

    def w_copy(k):
        return pltpu.make_async_copy(conv_w.at[k], wbuf.at[k], w_sem.at[k])

    small = [
        pltpu.make_async_copy(a, b, p_sem.at[i])
        for i, (a, b) in enumerate([(norm_g, gbuf), (norm_b, bbuf), (conv_b, cbuf), (attn_b, abuf)])
    ]
    aw_copy = pltpu.make_async_copy(attn_w, awbuf, p_sem.at[4])
    for f in range(2):
        x_copy(f).start()
    for c in small:
        c.start()
    barrier = pltpu.get_barrier_semaphore()
    for d in range(1, n):
        pl.semaphore_signal(barrier, inc=1, device_id={"time": lax.rem(me + d, n)}, device_id_type=MESH)

    zero_row = jnp.zeros((width, chans), jnp.bfloat16)
    for u in umaps:
        u[0:width, :] = zero_row
        u[width + pos : 2 * width + pos, :] = zero_row

    def put_stats(index, s1, s2):
        rows = [jnp.sum(s[:, 128 * b : 128 * b + 128], axis=0, keepdims=True) for s in (s1, s2) for b in range(lanes)]
        rows.append(jnp.zeros((8 - 2 * lanes, 128), jnp.float32))
        stat_out[index] = jnp.concatenate(rows, axis=0)

    def add_stats(carry, v):
        s1, s2 = carry
        t = v.reshape(v.shape[0] // 8, 8, v.shape[1])
        return s1 + jnp.sum(t, axis=0), s2 + jnp.sum(t * t, axis=0)

    zero_stats = (jnp.zeros((8, chans), jnp.float32),) * 2

    def stat_copy(index, d):
        return pltpu.make_async_remote_copy(
            src_ref=stat_out.at[index],
            dst_ref=stat_in.at[index, me],
            send_sem=st_send.at[index, d],
            recv_sem=st_recv.at[index, d],
            device_id={"time": lax.rem(me + d, n)},
            device_id_type=MESH,
        )

    def norm_params(index, sent=None):
        for d in range(1, n):
            stat_copy(index, d).start()
        if sent is not None:
            sent()
        stat_in[index, me] = stat_out[index]
        for d in range(1, n):
            stat_copy(index, d).wait()
        total = stat_in[index, 0]
        for d in range(1, n):
            total = total + stat_in[index, d]
        lane = lax.broadcasted_iota(jnp.int32, (8, 128), 1)
        chan = lane + 128 * lax.rem(lax.broadcasted_iota(jnp.int32, (8, 128), 0), lanes)
        place = lax.rem(chan, group)
        sums = jnp.zeros((8, 128), jnp.float32)
        for s in range(1 - group, group):
            moved = pltpu.roll(total, (-s) % 128, 1) if s else total
            if s > 0:
                moved = jnp.where(lane >= 128 - s, pltpu.roll(moved, 7, 0), moved)
            elif s < 0:
                moved = jnp.where(lane < -s, pltpu.roll(moved, 1, 0), moved)
            sums = sums + jnp.where((place + s >= 0) & (place + s < group), moved, 0.0)
        mean = jnp.concatenate([sums[b : b + 1] for b in range(lanes)], axis=1) / elems
        square = jnp.concatenate([sums[lanes + b : lanes + b + 1] for b in range(lanes)], axis=1) / elems
        scale = lax.rsqrt(square - mean * mean + NORM_EPS) * gbuf[pl.ds(index, 1), :]
        return mean, scale, bbuf[pl.ds(index, 1), :]

    def normed(v, params):
        mean, scale, shift = params
        return (v.astype(jnp.float32) - mean) * scale + shift

    def activate(v, params):
        y = 0.5 * normed(v, params)
        return (y + y * jnp.tanh(y)).astype(jnp.bfloat16)

    def fill(u, read, params):
        for i in range(height):
            u[(i + 1) * width : (i + 2) * width, :] = activate(read(i * width), params)

    def own(f):
        return lambda at: src[f, at : at + width, :]

    def halo(k, f):
        return lambda at: jnp.where(me == 0, src[0, at : at + width, :], land[k, f, at : at + width, :])

    early = 2 * width
    parts = ((1, 0, early), (1, early, pos - early), (0, 0, pos))

    def halo_copy(k, part):
        f, at, rows = parts[part]
        return pltpu.make_async_remote_copy(
            src_ref=src.at[f, pl.ds(at, rows)],
            dst_ref=land.at[k, f, pl.ds(at, rows)],
            send_sem=halo_send.at[k, part],
            recv_sem=halo_recv.at[k, part],
            device_id={"time": lax.min(me + 1, n - 1)},
            device_id_type=MESH,
        )

    def send_halo(k, *which):
        @pl.when(me < n - 1)
        def _():
            for part in which:
                halo_copy(k, part).start()

    def halo_sent(k, *which):
        @pl.when(me < n - 1)
        def _():
            for part in which:
                halo_copy(k, part).wait_send()

    def halo_here(k, *which):
        @pl.when(me > 0)
        def _():
            for part in which:
                halo_copy(k, part).wait_recv()

    column = lax.broadcasted_iota(jnp.int32, (width, 1), 0)

    spans = ((1, height - 1, (0, 1, 2)), (0, 1, (1, 2)), (height - 1, height, (0, 1)))

    def lhs(span, *us):
        top, end, ds = span
        return jnp.concatenate([u[(d + top) * width : (d + end) * width, :] for u in us for d in ds], axis=1)

    def rhs(span, k, a, e):
        return jnp.concatenate([wbuf[k, a * 9 + d * 3 + e] for d in span[2]], axis=0)

    def add_shifted(span, part, e, cols, first=False):
        for i in range(span[0], span[1]):
            at = slice(i * width, (i + 1) * width)
            v = part[(i - span[0]) * width : (i - span[0] + 1) * width]
            if e == 0:
                v = jnp.where(column == 0, 0.0, pltpu.roll(v, 1, 0))
            elif e == 2:
                v = jnp.where(column == width - 1, 0.0, pltpu.roll(v, width - 1, 0))
            acc[at, cols] = v if first else acc[at, cols] + v

    outs = [slice(o * chans, (o + 1) * chans) for o in range(2)]

    def one_out(k, u, a, o, first):
        for span in spans:
            part = dot(lhs(span, u), jnp.concatenate([rhs(span, k, a, e) for e in range(3)], axis=1))
            for e in range(3):
                add_shifted(span, part[:, e * chans : (e + 1) * chans], e, outs[o], first and e == 0)

    def both_outs(k, e, *frames, first=False):
        for span in spans:
            w = [jnp.concatenate([rhs(span, k, 2 - f, e), rhs(span, k, 1 - f, e)], axis=1) for f in frames]
            part = dot(lhs(span, *((u_0, u_m1)[f] for f in frames)), jnp.concatenate(w, axis=0))
            for o in range(2):
                add_shifted(span, part[:, outs[o]], e, outs[o], o == 0 and first)

    def finish(k, o, stats):
        bias = cbuf[pl.ds(k, 1), :]
        odd = lax.rem(k, 2) == 1
        for i in range(height):
            at = slice(i * width, (i + 1) * width)
            h = (acc[at, outs[o]] + bias).astype(jnp.bfloat16).astype(jnp.float32)
            old = xres[o, at, :]
            new = jnp.where(odd, h + old.astype(jnp.float32), h).astype(jnp.bfloat16)
            src[o, at, :] = new
            xres[o, at, :] = jnp.where(odd, new, old)
            stats = add_stats(stats, new.astype(jnp.float32))
        return stats

    def attention():
        params = norm_params(2)
        aw_copy.wait()
        part_rows = pos // 3

        def frame(t, carry):
            f = 1 - t

            def project(i, _):
                at = pl.ds(pl.multiple_of(i * part_rows, part_rows), part_rows)
                a = normed(xres[f, at, :], params).astype(jnp.bfloat16)
                w = jnp.concatenate([awbuf[0], awbuf[1], awbuf[2]], axis=1)
                b = jnp.concatenate([abuf[j : j + 1] for j in range(3)], axis=1)
                qkv[at, :] = (dot(a, w) + b).astype(jnp.bfloat16)
                return 0

            lax.fori_loop(0, 3, project, 0)

            def attend(i, carry):
                at = pl.ds(pl.multiple_of(i * part_rows, part_rows), part_rows)
                scores = lax.dot_general(
                    qkv[at, 0:chans], qkv[:, chans : 2 * chans], (((1,), (1,)), ((), ())), preferred_element_type=jnp.float32
                ) * chans ** -0.5
                top = jnp.max(scores, axis=1, keepdims=True)
                e = jnp.exp(scores - top)
                p = (e / jnp.sum(e, axis=1, keepdims=True)).astype(jnp.bfloat16)
                o = dot(p, qkv[:, 2 * chans : 3 * chans]).astype(jnp.bfloat16)
                h = (dot(o, awbuf[3]) + abuf[3:4]).astype(jnp.bfloat16)
                new = (xres[f, at, :].astype(jnp.float32) + h.astype(jnp.float32)).astype(jnp.bfloat16)
                src[f, at, :] = new
                xres[f, at, :] = new
                return add_stats(carry, new.astype(jnp.float32))

            carry = lax.fori_loop(0, 3, attend, carry)

            @pl.when(t == 0)
            def _():
                send_halo(2, 0)

            return carry

        put_stats(3, *lax.fori_loop(0, 2, frame, zero_stats))

    for f in range(2):
        x_copy(f).wait()
    for c in small:
        c.wait()
    for k in range(4):
        w_copy(k).start()
    aw_copy.start()

    def first_row(i, carry):
        for f in range(2):
            at = pl.ds(pl.multiple_of(i * width, width), width)
            v = src[f, at, :]
            xres[f, at, :] = v
            carry = add_stats(carry, v.astype(jnp.float32))
        return carry

    put_stats(0, *lax.fori_loop(0, height, first_row, zero_stats))
    pl.semaphore_wait(barrier, n - 1)
    send_halo(0, 0)

    def stage(k, _):
        index = k + lax.div(k, 2)
        params = norm_params(index, lambda: send_halo(k, 1, 2))
        fill(u_1, own(1), params)
        w_copy(k).wait()
        fill(u_0, own(0), params)
        one_out(k, u_1, 2, 1, True)
        both_outs(k, 0, 0, first=True)
        both_outs(k, 1, 0)
        halo_here(k, 0, 1)
        fill(u_m1, halo(k, 1), params)
        both_outs(k, 2, 0)
        both_outs(k, 0, 1)
        both_outs(k, 1, 1)
        halo_here(k, 2)
        fill(u_m2, halo(k, 0), params)
        both_outs(k, 2, 1)
        halo_sent(k, 0, 1)
        stats = finish(k, 1, zero_stats)

        @pl.when(lax.rem(k, 2) == 0)
        def _():
            send_halo(k + 1, 0)

        one_out(k, u_m2, 0, 0, False)
        halo_sent(k, 2)
        stats = finish(k, 0, stats)
        put_stats(lax.min(index + 1, 4), *stats)

        @pl.when(k == 1)
        def _():
            attention()

        return 0

    lax.fori_loop(0, 4, stage, 0)
    out[...] = src[...]


def solution(mesh):
    n = mesh.shape["time"]
    video_spec = P(("batch", "time"), None, None, None)

    def device_body(latent, conv_w, conv_b, norm_g, norm_b, attn_w, attn_b):
        frames, height, width, chans = latent.shape
        pos = height * width
        bf16, f32 = jnp.bfloat16, jnp.float32
        out = pl.pallas_call(
            functools.partial(block_kernel, n, height, width, chans),
            out_shape=jax.ShapeDtypeStruct((frames, pos, chans), bf16),
            in_specs=[pl.BlockSpec(memory_space=pl.ANY)] * 7,
            out_specs=pl.BlockSpec(memory_space=pltpu.VMEM),
            scratch_shapes=[
                pltpu.VMEM((4, 27, chans, chans), bf16),
                pltpu.VMEM((4, chans, chans), bf16),
                pltpu.VMEM((4, chans), f32),
                pltpu.VMEM((5, chans), f32),
                pltpu.VMEM((5, chans), f32),
                pltpu.VMEM((4, chans), f32),
                pltpu.VMEM((pos + 2 * width, chans), bf16),
                pltpu.VMEM((pos + 2 * width, chans), bf16),
                pltpu.VMEM((pos + 2 * width, chans), bf16),
                pltpu.VMEM((pos + 2 * width, chans), bf16),
                pltpu.VMEM((2, pos, chans), bf16),
                pltpu.VMEM((2, pos, chans), bf16),
                pltpu.VMEM((4, 2, pos, chans), bf16),
                pltpu.VMEM((pos, 2 * chans), f32),
                pltpu.VMEM((pos, 3 * chans), bf16),
                pltpu.VMEM((5, 8, 128), f32),
                pltpu.VMEM((5, n, 8, 128), f32),
                pltpu.SemaphoreType.DMA((4,)),
                pltpu.SemaphoreType.DMA((5,)),
                pltpu.SemaphoreType.DMA((2,)),
                pltpu.SemaphoreType.DMA((4, 3)),
                pltpu.SemaphoreType.DMA((4, 3)),
                pltpu.SemaphoreType.DMA((5, n)),
                pltpu.SemaphoreType.DMA((5, n)),
            ],
            compiler_params=pltpu.CompilerParams(collective_id=0, has_side_effects=True, vmem_limit_bytes=55000000),
            name="mid_block",
        )(*(pltpu.with_memory_space_constraint(x, pltpu.HBM) for x in (latent.reshape(frames, pos, chans), conv_w.reshape(4, 27, chans, chans), conv_b, norm_g, norm_b, attn_w, attn_b)))
        return out.reshape(latent.shape)

    return jax.shard_map(device_body, mesh=mesh, in_specs=(video_spec, P(), P(), P(), P(), P(), P()), out_specs=video_spec, check_vma=False)
```

```python
import functools

import jax
import jax.numpy as jnp
from jax import lax
from jax.experimental import pallas as pl
from jax.experimental.pallas import tpu as pltpu
from jax.sharding import PartitionSpec as P

GROUPS = 32
NORM_EPS = 1e-6
LOG2E = 1.4426950408889634
MESH = pl.DeviceIdType.MESH


def dot(a, b):
    return jnp.dot(a, b, preferred_element_type=jnp.float32)


def copy_kernel(a, out, sem):
    c = pltpu.make_async_copy(a, out, sem)
    c.start()
    c.wait()


def block_kernel(
    n, height, width, chans,
    latent, conv_w, conv_b, norm_g, norm_b, attn_w, attn_b, out,
    wbuf, awbuf, cbuf, gbuf, bbuf, abuf, u_m2, u_m1, u_0, u_1, src, xres, land, acc, qkv, stat_out, stat_in,
    w_sem, p_sem, x_sem, halo_send, halo_recv, st_send, st_recv,
):
    pos = height * width
    taps = 27
    lanes = chans // 128
    group = chans // GROUPS
    elems = n * 2 * pos * group
    me = lax.axis_index("time")
    umaps = (u_m2, u_m1, u_0, u_1)

    def x_copy(f):
        return pltpu.make_async_copy(latent.at[f], src.at[f], x_sem.at[f])

    def w_copy(k):
        return pltpu.make_async_copy(conv_w.at[k], wbuf.at[k], w_sem.at[k])

    small = [
        pltpu.make_async_copy(a, b, p_sem.at[i])
        for i, (a, b) in enumerate([(norm_g, gbuf), (norm_b, bbuf), (conv_b, cbuf), (attn_b, abuf)])
    ]
    aw_copy = pltpu.make_async_copy(attn_w, awbuf, p_sem.at[4])
    for f in range(2):
        x_copy(f).start()
    for c in small:
        c.start()
    barrier = pltpu.get_barrier_semaphore()
    for d in range(1, n):
        pl.semaphore_signal(barrier, inc=1, device_id={"time": lax.rem(me + d, n)}, device_id_type=MESH)

    zero_row = jnp.zeros((width, chans), jnp.bfloat16)
    for u in umaps:
        u[0:width, :] = zero_row
        u[width + pos : 2 * width + pos, :] = zero_row

    def put_stats(index, s1, s2):
        rows = [jnp.sum(s[:, 128 * b : 128 * b + 128], axis=0, keepdims=True) for s in (s1, s2) for b in range(lanes)]
        rows.append(jnp.zeros((8 - 2 * lanes, 128), jnp.float32))
        stat_out[index] = jnp.concatenate(rows, axis=0)

    def add_stats(carry, v):
        s1, s2 = carry
        t = v.reshape(v.shape[0] // 8, 8, v.shape[1])
        return s1 + jnp.sum(t, axis=0), s2 + jnp.sum(t * t, axis=0)

    zero_stats = (jnp.zeros((8, chans), jnp.float32),) * 2

    def stat_copy(index, d):
        return pltpu.make_async_remote_copy(
            src_ref=stat_out.at[index],
            dst_ref=stat_in.at[index, me],
            send_sem=st_send.at[index, d],
            recv_sem=st_recv.at[index, d],
            device_id={"time": lax.rem(me + d, n)},
            device_id_type=MESH,
        )

    def norm_params(index, sent=None):
        for d in range(1, n):
            stat_copy(index, d).start()
        if sent is not None:
            sent()
        stat_in[index, me] = stat_out[index]
        for d in range(1, n):
            stat_copy(index, d).wait()
        total = stat_in[index, 0]
        for d in range(1, n):
            total = total + stat_in[index, d]
        lane = lax.broadcasted_iota(jnp.int32, (8, 128), 1)
        chan = lane + 128 * lax.rem(lax.broadcasted_iota(jnp.int32, (8, 128), 0), lanes)
        place = lax.rem(chan, group)
        sums = jnp.zeros((8, 128), jnp.float32)
        for s in range(1 - group, group):
            moved = pltpu.roll(total, (-s) % 128, 1) if s else total
            if s > 0:
                moved = jnp.where(lane >= 128 - s, pltpu.roll(moved, 7, 0), moved)
            elif s < 0:
                moved = jnp.where(lane < -s, pltpu.roll(moved, 1, 0), moved)
            sums = sums + jnp.where((place + s >= 0) & (place + s < group), moved, 0.0)
        mean = jnp.concatenate([sums[b : b + 1] for b in range(lanes)], axis=1) / elems
        square = jnp.concatenate([sums[lanes + b : lanes + b + 1] for b in range(lanes)], axis=1) / elems
        scale = lax.rsqrt(square - mean * mean + NORM_EPS) * gbuf[pl.ds(index, 1), :]
        return mean, scale, bbuf[pl.ds(index, 1), :]

    def normed(v, params):
        mean, scale, shift = params
        return (v.astype(jnp.float32) - mean) * scale + shift

    def activate(v, params):
        y = 0.5 * normed(v, params)
        return (y + y * jnp.tanh(y)).astype(jnp.bfloat16)

    def fill(u, read, params):
        for i in range(height):
            u[(i + 1) * width : (i + 2) * width, :] = activate(read(i * width), params)

    def own(f):
        return lambda at: src[f, at : at + width, :]

    def halo(k, f):
        return lambda at: jnp.where(me == 0, src[0, at : at + width, :], land[k, f, at : at + width, :])

    early = 3 * width
    parts = ((1, 0, early), (1, early, pos - early), (0, 0, pos))

    def halo_copy(k, part):
        f, at, rows = parts[part]
        return pltpu.make_async_remote_copy(
            src_ref=src.at[f, pl.ds(at, rows)],
            dst_ref=land.at[k, f, pl.ds(at, rows)],
            send_sem=halo_send.at[k, part],
            recv_sem=halo_recv.at[k, part],
            device_id={"time": lax.min(me + 1, n - 1)},
            device_id_type=MESH,
        )

    def send_halo(k, *which):
        @pl.when(me < n - 1)
        def _():
            for part in which:
                halo_copy(k, part).start()

    def halo_sent(k, *which):
        @pl.when(me < n - 1)
        def _():
            for part in which:
                halo_copy(k, part).wait_send()

    def halo_here(k, *which):
        @pl.when(me > 0)
        def _():
            for part in which:
                halo_copy(k, part).wait_recv()

    column = lax.broadcasted_iota(jnp.int32, (width, 1), 0)

    spans = ((1, height - 1, (0, 1, 2)), (0, 1, (1, 2)), (height - 1, height, (0, 1)))

    def lhs(span, *us):
        top, end, ds = span
        return jnp.concatenate([u[(d + top) * width : (d + end) * width, :] for u in us for d in ds], axis=1)

    def rhs(span, k, a, e):
        return jnp.concatenate([wbuf[k, a * 9 + d * 3 + e] for d in span[2]], axis=0)

    def add_shifted(span, part, e, cols, first=False):
        for i in range(span[0], span[1]):
            at = slice(i * width, (i + 1) * width)
            v = part[(i - span[0]) * width : (i - span[0] + 1) * width]
            if e == 0:
                v = jnp.where(column == 0, 0.0, pltpu.roll(v, 1, 0))
            elif e == 2:
                v = jnp.where(column == width - 1, 0.0, pltpu.roll(v, width - 1, 0))
            acc[at, cols] = v if first else acc[at, cols] + v

    outs = [slice(o * chans, (o + 1) * chans) for o in range(2)]

    def one_out(k, frames, o, first):
        for span in spans:
            w = [jnp.concatenate([rhs(span, k, a, e) for e in range(3)], axis=1) for _, a in frames]
            part = dot(lhs(span, *(u for u, _ in frames)), jnp.concatenate(w, axis=0))
            for e in range(3):
                add_shifted(span, part[:, e * chans : (e + 1) * chans], e, outs[o], first and e == 0)

    def both_outs(k, e, *frames, first=False):
        for span in spans:
            w = [jnp.concatenate([rhs(span, k, 2 - f, e), rhs(span, k, 1 - f, e)], axis=1) for f in frames]
            part = dot(lhs(span, *((u_0, u_m1)[f] for f in frames)), jnp.concatenate(w, axis=0))
            for o in range(2):
                add_shifted(span, part[:, outs[o]], e, outs[o], o == 0 and first)

    def finish(k, o, stats):
        bias = cbuf[pl.ds(k, 1), :]
        odd = lax.rem(k, 2) == 1
        for i in range(height):
            at = slice(i * width, (i + 1) * width)
            h = (acc[at, outs[o]] + bias).astype(jnp.bfloat16).astype(jnp.float32)
            old = xres[o, at, :]
            new = jnp.where(odd, h + old.astype(jnp.float32), h).astype(jnp.bfloat16)
            src[o, at, :] = new
            xres[o, at, :] = jnp.where(odd, new, old)
            stats = add_stats(stats, new.astype(jnp.float32))
        return stats

    def attention():
        params = norm_params(2)
        aw_copy.wait()
        rows = pos // 3
        w = jnp.concatenate([awbuf[j] for j in range(3)], axis=1)
        b = jnp.concatenate([abuf[j : j + 1] for j in range(3)], axis=1)
        for f in (1, 0):
            u = (u_0, u_1)[f]
            for i in range(height):
                at = slice(i * width, (i + 1) * width)
                u[at, :] = normed(xres[f, at, :], params).astype(jnp.bfloat16)
            qkv[f] = (dot(u[0:pos, :], w) + b).astype(jnp.bfloat16)
        stats = zero_stats
        for f in (1, 0):
            for i in range(3):
                at = slice(i * rows, (i + 1) * rows)
                scores = lax.dot_general(
                    qkv[f, at, 0:chans], qkv[f, :, chans : 2 * chans], (((1,), (1,)), ((), ())), preferred_element_type=jnp.float32
                )
                top = jnp.max(scores, axis=1, keepdims=True)
                e = jnp.exp2((scores - top) * (chans ** -0.5 * LOG2E))
                p = (e * (1.0 / jnp.sum(e, axis=1, keepdims=True))).astype(jnp.bfloat16)
                o = dot(p, qkv[f, :, 2 * chans : 3 * chans]).astype(jnp.bfloat16)
                h = (dot(o, awbuf[3]) + abuf[3:4]).astype(jnp.bfloat16)
                new = (xres[f, at, :].astype(jnp.float32) + h.astype(jnp.float32)).astype(jnp.bfloat16)
                src[f, at, :] = new
                xres[f, at, :] = new
                stats = add_stats(stats, new.astype(jnp.float32))
            if f == 1:
                send_halo(2, 0)
        put_stats(3, *stats)
        for u in (u_0, u_1):
            u[0:width, :] = jnp.zeros((width, chans), jnp.bfloat16)

    for f in range(2):
        x_copy(f).wait()
    for c in small:
        c.wait()
    for k in range(4):
        w_copy(k).start()
    aw_copy.start()

    def first_row(i, carry):
        for f in range(2):
            at = pl.ds(pl.multiple_of(i * width, width), width)
            v = src[f, at, :]
            xres[f, at, :] = v
            carry = add_stats(carry, v.astype(jnp.float32))
        return carry

    put_stats(0, *lax.fori_loop(0, height, first_row, zero_stats))
    pl.semaphore_wait(barrier, n - 1)
    send_halo(0, 0)

    def stage(k, _):
        index = k + lax.div(k, 2)
        params = norm_params(index, lambda: send_halo(k, 1, 2))
        w_copy(k).wait()
        fill(u_1, own(1), params)
        fill(u_0, own(0), params)
        one_out(k, ((u_1, 2),), 1, True)
        both_outs(k, 0, 0, first=True)
        both_outs(k, 1, 0)
        halo_here(k, 0, 1)
        fill(u_m1, halo(k, 1), params)
        both_outs(k, 2, 0)
        one_out(k, ((u_m1, 0),), 1, False)
        halo_sent(k, 0, 1)
        stats = finish(k, 1, zero_stats)

        @pl.when(lax.rem(k, 2) == 0)
        def _():
            send_halo(k + 1, 0)

        halo_here(k, 2)
        fill(u_m2, halo(k, 0), params)
        one_out(k, ((u_m1, 1), (u_m2, 0)), 0, False)
        halo_sent(k, 2)
        stats = finish(k, 0, stats)
        put_stats(lax.min(index + 1, 4), *stats)

        @pl.when(k == 1)
        def _():
            attention()

        return 0

    lax.fori_loop(0, 4, stage, 0)
    out[...] = src[...]


def solution(mesh):
    n = mesh.shape["time"]
    video_spec = P(("batch", "time"), None, None, None)

    def device_body(latent, conv_w, conv_b, norm_g, norm_b, attn_w, attn_b):
        frames, height, width, chans = latent.shape
        pos = height * width
        bf16, f32 = jnp.bfloat16, jnp.float32
        out = pl.pallas_call(
            functools.partial(block_kernel, n, height, width, chans),
            out_shape=jax.ShapeDtypeStruct((frames, pos, chans), bf16),
            in_specs=[pl.BlockSpec(memory_space=pl.ANY)] * 7,
            out_specs=pl.BlockSpec(memory_space=pltpu.VMEM),
            scratch_shapes=[
                pltpu.VMEM((4, 27, chans, chans), bf16),
                pltpu.VMEM((4, chans, chans), bf16),
                pltpu.VMEM((4, chans), f32),
                pltpu.VMEM((5, chans), f32),
                pltpu.VMEM((5, chans), f32),
                pltpu.VMEM((4, chans), f32),
                pltpu.VMEM((pos + 2 * width, chans), bf16),
                pltpu.VMEM((pos + 2 * width, chans), bf16),
                pltpu.VMEM((pos + 2 * width, chans), bf16),
                pltpu.VMEM((pos + 2 * width, chans), bf16),
                pltpu.VMEM((2, pos, chans), bf16),
                pltpu.VMEM((2, pos, chans), bf16),
                pltpu.VMEM((4, 2, pos, chans), bf16),
                pltpu.VMEM((pos, 2 * chans), f32),
                pltpu.VMEM((2, pos, 3 * chans), bf16),
                pltpu.VMEM((5, 8, 128), f32),
                pltpu.VMEM((5, n, 8, 128), f32),
                pltpu.SemaphoreType.DMA((4,)),
                pltpu.SemaphoreType.DMA((5,)),
                pltpu.SemaphoreType.DMA((2,)),
                pltpu.SemaphoreType.DMA((4, 3)),
                pltpu.SemaphoreType.DMA((4, 3)),
                pltpu.SemaphoreType.DMA((5, n)),
                pltpu.SemaphoreType.DMA((5, n)),
            ],
            compiler_params=pltpu.CompilerParams(collective_id=0, has_side_effects=True, vmem_limit_bytes=55000000),
            name="mid_block",
        )(*(pltpu.with_memory_space_constraint(x, pltpu.HBM) for x in (latent.reshape(frames, pos, chans), conv_w.reshape(4, 27, chans, chans), conv_b, norm_g, norm_b, attn_w, attn_b)))
        return out.reshape(latent.shape)

    return jax.shard_map(device_body, mesh=mesh, in_specs=(video_spec, P(), P(), P(), P(), P(), P()), out_specs=video_spec, check_vma=False)
```

```python
import functools

import jax
import jax.numpy as jnp
from jax import lax
from jax.experimental import pallas as pl
from jax.experimental.pallas import tpu as pltpu
from jax.sharding import PartitionSpec as P

GROUPS = 32
NORM_EPS = 1e-6
LOG2E = 1.4426950408889634
MESH = pl.DeviceIdType.MESH


def dot(a, b):
    return jnp.dot(a, b, preferred_element_type=jnp.float32)


def copy_kernel(a, out, sem):
    c = pltpu.make_async_copy(a, out, sem)
    c.start()
    c.wait()


def block_kernel(
    n, height, width, chans,
    latent, conv_w, conv_b, norm_g, norm_b, attn_w, attn_b, out,
    wbuf, awbuf, cbuf, gbuf, bbuf, abuf, u_m2, u_m1, u_0, u_1, src, xres, land, acc, qkv, stat_out, stat_in,
    w_sem, p_sem, x_sem, halo_send, halo_recv, st_send, st_recv,
):
    pos = height * width
    taps = 27
    lanes = chans // 128
    group = chans // GROUPS
    elems = n * 2 * pos * group
    me = lax.axis_index("time")
    umaps = (u_m2, u_m1, u_0, u_1)

    def x_copy(f):
        return pltpu.make_async_copy(latent.at[f], src.at[f], x_sem.at[f])

    def w_copy(k):
        return pltpu.make_async_copy(conv_w.at[k], wbuf.at[k], w_sem.at[k])

    small = [
        pltpu.make_async_copy(a, b, p_sem.at[i])
        for i, (a, b) in enumerate([(norm_g, gbuf), (norm_b, bbuf), (conv_b, cbuf), (attn_b, abuf)])
    ]
    aw_copy = pltpu.make_async_copy(attn_w, awbuf, p_sem.at[4])
    for f in range(2):
        x_copy(f).start()
    for c in small:
        c.start()
    barrier = pltpu.get_barrier_semaphore()
    for d in range(1, n):
        pl.semaphore_signal(barrier, inc=1, device_id={"time": lax.rem(me + d, n)}, device_id_type=MESH)

    zero_row = jnp.zeros((width, chans), jnp.bfloat16)
    for u in umaps:
        u[0:width, :] = zero_row
        u[width + pos : 2 * width + pos, :] = zero_row

    def put_stats(index, s1, s2):
        rows = [jnp.sum(s[:, 128 * b : 128 * b + 128], axis=0, keepdims=True) for s in (s1, s2) for b in range(lanes)]
        rows.append(jnp.zeros((8 - 2 * lanes, 128), jnp.float32))
        stat_out[index] = jnp.concatenate(rows, axis=0)

    def add_stats(carry, v):
        s1, s2 = carry
        t = v.reshape(v.shape[0] // 8, 8, v.shape[1])
        return s1 + jnp.sum(t, axis=0), s2 + jnp.sum(t * t, axis=0)

    zero_stats = (jnp.zeros((8, chans), jnp.float32),) * 2

    def stat_copy(index, d):
        return pltpu.make_async_remote_copy(
            src_ref=stat_out.at[index],
            dst_ref=stat_in.at[index, me],
            send_sem=st_send.at[index, d],
            recv_sem=st_recv.at[index, d],
            device_id={"time": lax.rem(me + d, n)},
            device_id_type=MESH,
        )

    def norm_params(index, sent=None):
        for d in range(1, n):
            stat_copy(index, d).start()
        if sent is not None:
            sent()
        stat_in[index, me] = stat_out[index]
        for d in range(1, n):
            stat_copy(index, d).wait()
        total = stat_in[index, 0]
        for d in range(1, n):
            total = total + stat_in[index, d]
        lane = lax.broadcasted_iota(jnp.int32, (8, 128), 1)
        chan = lane + 128 * lax.rem(lax.broadcasted_iota(jnp.int32, (8, 128), 0), lanes)
        place = lax.rem(chan, group)
        sums = jnp.zeros((8, 128), jnp.float32)
        for s in range(1 - group, group):
            moved = pltpu.roll(total, (-s) % 128, 1) if s else total
            if s > 0:
                moved = jnp.where(lane >= 128 - s, pltpu.roll(moved, 7, 0), moved)
            elif s < 0:
                moved = jnp.where(lane < -s, pltpu.roll(moved, 1, 0), moved)
            sums = sums + jnp.where((place + s >= 0) & (place + s < group), moved, 0.0)
        mean = jnp.concatenate([sums[b : b + 1] for b in range(lanes)], axis=1) / elems
        square = jnp.concatenate([sums[lanes + b : lanes + b + 1] for b in range(lanes)], axis=1) / elems
        scale = lax.rsqrt(square - mean * mean + NORM_EPS) * gbuf[pl.ds(index, 1), :]
        return mean, scale, bbuf[pl.ds(index, 1), :]

    def normed(v, params):
        mean, scale, shift = params
        return (v.astype(jnp.float32) - mean) * scale + shift

    def activate(v, params):
        y = 0.5 * normed(v, params)
        return (y + y * jnp.tanh(y)).astype(jnp.bfloat16)

    def fill(u, read, params):
        for i in range(height):
            u[(i + 1) * width : (i + 2) * width, :] = activate(read(i * width), params)

    def own(f):
        return lambda at: src[f, at : at + width, :]

    def halo(k, f):
        return lambda at: jnp.where(me == 0, src[0, at : at + width, :], land[k, f, at : at + width, :])

    early = 3 * width
    parts = ((1, 0, early), (1, early, pos - early), (0, 0, pos))

    def halo_copy(k, part):
        f, at, rows = parts[part]
        return pltpu.make_async_remote_copy(
            src_ref=src.at[f, pl.ds(at, rows)],
            dst_ref=land.at[k, f, pl.ds(at, rows)],
            send_sem=halo_send.at[k, part],
            recv_sem=halo_recv.at[k, part],
            device_id={"time": lax.min(me + 1, n - 1)},
            device_id_type=MESH,
        )

    def send_halo(k, *which):
        @pl.when(me < n - 1)
        def _():
            for part in which:
                halo_copy(k, part).start()

    def halo_sent(k, *which):
        @pl.when(me < n - 1)
        def _():
            for part in which:
                halo_copy(k, part).wait_send()

    def halo_here(k, *which):
        @pl.when(me > 0)
        def _():
            for part in which:
                halo_copy(k, part).wait_recv()

    column = lax.broadcasted_iota(jnp.int32, (width, 1), 0)

    spans = ((1, height - 1, (0, 1, 2)), (0, 1, (1, 2)), (height - 1, height, (0, 1)))

    def lhs(span, *us):
        top, end, ds = span
        return jnp.concatenate([u[(d + top) * width : (d + end) * width, :] for u in us for d in ds], axis=1)

    def rhs(span, k, a, e):
        return jnp.concatenate([wbuf[k, a * 9 + d * 3 + e] for d in span[2]], axis=0)

    def add_shifted(span, part, e, cols, first=False):
        for i in range(span[0], span[1]):
            at = slice(i * width, (i + 1) * width)
            v = part[(i - span[0]) * width : (i - span[0] + 1) * width]
            if e == 0:
                v = jnp.where(column == 0, 0.0, pltpu.roll(v, 1, 0))
            elif e == 2:
                v = jnp.where(column == width - 1, 0.0, pltpu.roll(v, width - 1, 0))
            acc[at, cols] = v if first else acc[at, cols] + v

    outs = [slice(o * chans, (o + 1) * chans) for o in range(2)]

    def one_out(k, frames, o, first):
        for span in (spans[1], spans[0], spans[2]) if first else spans:
            w = [jnp.concatenate([rhs(span, k, a, e) for e in range(3)], axis=1) for _, a in frames]
            part = dot(lhs(span, *(u for u, _ in frames)), jnp.concatenate(w, axis=0))
            for e in range(3):
                add_shifted(span, part[:, e * chans : (e + 1) * chans], e, outs[o], first and e == 0)

    def both_outs(k, e, *frames, first=False):
        for span in spans:
            w = [jnp.concatenate([rhs(span, k, 2 - f, e), rhs(span, k, 1 - f, e)], axis=1) for f in frames]
            part = dot(lhs(span, *((u_0, u_m1)[f] for f in frames)), jnp.concatenate(w, axis=0))
            for o in range(2):
                add_shifted(span, part[:, outs[o]], e, outs[o], o == 0 and first)

    def finish(k, o, stats):
        bias = cbuf[pl.ds(k, 1), :]
        odd = lax.rem(k, 2) == 1
        for i in range(height):
            at = slice(i * width, (i + 1) * width)
            h = (acc[at, outs[o]] + bias).astype(jnp.bfloat16).astype(jnp.float32)
            old = xres[o, at, :]
            new = jnp.where(odd, h + old.astype(jnp.float32), h).astype(jnp.bfloat16)
            src[o, at, :] = new
            xres[o, at, :] = jnp.where(odd, new, old)
            stats = add_stats(stats, new.astype(jnp.float32))
        return stats

    def attention():
        params = norm_params(2)
        aw_copy.wait()
        rows = pos // 3
        w = jnp.concatenate([awbuf[j] for j in range(3)], axis=1)
        b = jnp.concatenate([abuf[j : j + 1] for j in range(3)], axis=1)
        for f in (1, 0):
            u = (u_0, u_1)[f]
            for i in range(height):
                at = slice(i * width, (i + 1) * width)
                u[at, :] = normed(xres[f, at, :], params).astype(jnp.bfloat16)
            qkv[f] = (dot(u[0:pos, :], w) + b).astype(jnp.bfloat16)
        stats = zero_stats
        for f in (1, 0):
            for i in range(3):
                at = slice(i * rows, (i + 1) * rows)
                scores = lax.dot_general(
                    qkv[f, at, 0:chans], qkv[f, :, chans : 2 * chans], (((1,), (1,)), ((), ())), preferred_element_type=jnp.float32
                )
                top = jnp.max(scores, axis=1, keepdims=True)
                e = jnp.exp2((scores - top) * (chans ** -0.5 * LOG2E))
                p = (e * (1.0 / jnp.sum(e, axis=1, keepdims=True))).astype(jnp.bfloat16)
                o = dot(p, qkv[f, :, 2 * chans : 3 * chans]).astype(jnp.bfloat16)
                h = (dot(o, awbuf[3]) + abuf[3:4]).astype(jnp.bfloat16)
                new = (xres[f, at, :].astype(jnp.float32) + h.astype(jnp.float32)).astype(jnp.bfloat16)
                src[f, at, :] = new
                xres[f, at, :] = new
                stats = add_stats(stats, new.astype(jnp.float32))
            if f == 1:
                send_halo(2, 0)
        put_stats(3, *stats)
        for u in (u_0, u_1):
            u[0:width, :] = jnp.zeros((width, chans), jnp.bfloat16)

    for f in range(2):
        x_copy(f).wait()
    for c in small:
        c.wait()
    w_copy(0).start()

    def first_row(i, carry):
        for f in range(2):
            at = pl.ds(pl.multiple_of(i * width, width), width)
            v = src[f, at, :]
            xres[f, at, :] = v
            carry = add_stats(carry, v.astype(jnp.float32))
        return carry

    put_stats(0, *lax.fori_loop(0, height, first_row, zero_stats))
    pl.semaphore_wait(barrier, n - 1)
    send_halo(0, 0)

    def stage(k, _):
        index = k + lax.div(k, 2)
        params = norm_params(index, lambda: send_halo(k, 1, 2))
        w_copy(k).wait()

        @pl.when(k < 3)
        def _():
            w_copy(lax.min(k + 1, 3)).start()

        @pl.when(k == 0)
        def _():
            aw_copy.start()

        fill(u_1, own(1), params)
        fill(u_0, own(0), params)
        one_out(k, ((u_1, 2),), 1, True)
        both_outs(k, 0, 0, first=True)
        both_outs(k, 1, 0)
        halo_here(k, 0, 1)
        fill(u_m1, halo(k, 1), params)
        both_outs(k, 2, 0)
        one_out(k, ((u_m1, 0),), 1, False)
        halo_sent(k, 0, 1)
        stats = finish(k, 1, zero_stats)

        @pl.when(lax.rem(k, 2) == 0)
        def _():
            send_halo(k + 1, 0)

        halo_here(k, 2)
        fill(u_m2, halo(k, 0), params)
        one_out(k, ((u_m1, 1), (u_m2, 0)), 0, False)
        halo_sent(k, 2)
        stats = finish(k, 0, stats)
        put_stats(lax.min(index + 1, 4), *stats)

        @pl.when(k == 1)
        def _():
            attention()

        return 0

    lax.fori_loop(0, 4, stage, 0)
    out[...] = src[...]


def solution(mesh):
    n = mesh.shape["time"]
    video_spec = P(("batch", "time"), None, None, None)

    def device_body(latent, conv_w, conv_b, norm_g, norm_b, attn_w, attn_b):
        frames, height, width, chans = latent.shape
        pos = height * width
        bf16, f32 = jnp.bfloat16, jnp.float32
        out = pl.pallas_call(
            functools.partial(block_kernel, n, height, width, chans),
            out_shape=jax.ShapeDtypeStruct((frames, pos, chans), bf16),
            in_specs=[pl.BlockSpec(memory_space=pl.ANY)] * 7,
            out_specs=pl.BlockSpec(memory_space=pltpu.VMEM),
            scratch_shapes=[
                pltpu.VMEM((4, 27, chans, chans), bf16),
                pltpu.VMEM((4, chans, chans), bf16),
                pltpu.VMEM((4, chans), f32),
                pltpu.VMEM((5, chans), f32),
                pltpu.VMEM((5, chans), f32),
                pltpu.VMEM((4, chans), f32),
                pltpu.VMEM((pos + 2 * width, chans), bf16),
                pltpu.VMEM((pos + 2 * width, chans), bf16),
                pltpu.VMEM((pos + 2 * width, chans), bf16),
                pltpu.VMEM((pos + 2 * width, chans), bf16),
                pltpu.VMEM((2, pos, chans), bf16),
                pltpu.VMEM((2, pos, chans), bf16),
                pltpu.VMEM((4, 2, pos, chans), bf16),
                pltpu.VMEM((pos, 2 * chans), f32),
                pltpu.VMEM((2, pos, 3 * chans), bf16),
                pltpu.VMEM((5, 8, 128), f32),
                pltpu.VMEM((5, n, 8, 128), f32),
                pltpu.SemaphoreType.DMA((4,)),
                pltpu.SemaphoreType.DMA((5,)),
                pltpu.SemaphoreType.DMA((2,)),
                pltpu.SemaphoreType.DMA((4, 3)),
                pltpu.SemaphoreType.DMA((4, 3)),
                pltpu.SemaphoreType.DMA((5, n)),
                pltpu.SemaphoreType.DMA((5, n)),
            ],
            compiler_params=pltpu.CompilerParams(collective_id=0, has_side_effects=True, vmem_limit_bytes=55000000),
            name="mid_block",
        )(*(pltpu.with_memory_space_constraint(x, pltpu.HBM) for x in (latent.reshape(frames, pos, chans), conv_w.reshape(4, 27, chans, chans), conv_b, norm_g, norm_b, attn_w, attn_b)))
        return out.reshape(latent.shape)

    return jax.shard_map(device_body, mesh=mesh, in_specs=(video_spec, P(), P(), P(), P(), P(), P()), out_specs=video_spec, check_vma=False)
```
